256 devices in a mesh: dp: 4 (over x), seq: 8 (over z_lo, core), head: 8 (over y, z_hi).
Axes of the slice: x: 4, y: 4, z: 8 (z_hi: 2, z_lo: 4; z = z_hi * 4 + z_lo), core: 2. Of those that a mesh axis runs over, the one named last changes fastest.
Arguments:
- q_lat: bfloat16 [12288, 8192], P(('dp', 'seq'), 'head'), may hold values from -160 to 160
- q_rope: bfloat16 [12288, 1024], P(('dp', 'seq'), 'head'), may hold values from -6 to 6
- grad_out: bfloat16 [12288, 8192], P(('dp', 'seq'), 'head'), may hold values from -6 to 6
- prefix_keys: bfloat16 [576, 2048], P(None, 'seq'), may hold values from -6 to 6
- comp_lengths: int32 [12], replicated, may hold values from 128 to 1024, as said below
- prefix_len: int32 [1], replicated, may hold values from 257 to 2048
Outputs:
- dq_lat: bfloat16 [12288, 8192], P(('dp', 'seq'), 'head')
- dq_rope: bfloat16 [12288, 1024], P(('dp', 'seq'), 'head')
- d_keys: float32 [576, 2048], P(None, ('seq', 'head'))
The draws below stay inside these ranges and needn't reach their ends.
Inputs may be any that keep to these rules, and one draw needn't show every extreme that they name: `comp_lengths`: each a multiple of 128.
All inputs are finite; a program needn't handle non-finite values.
Results may differ from the reference program's by a relative error of at most 0.0089.
Values may be sent and summed in bfloat16 or wider, within the bound.
No kernel may reach another device: no remote copies, remote signals or barrier semaphores. Data moves between devices by JAX's collectives and lax.ppermute only.
A program may use at most 64 MiB of HBM per device.

```python
import jax
import jax.numpy as jnp
from jax import lax

H = 16
DL = 512
DR = 64
CLEN = 1024
LBLK = 128
TOKENS = 12288
P_SIZE = 2048
COMPS = 12


def key_matrix(key):
    values = jax.random.normal(jax.random.fold_in(key, 7001), (DL + DR, P_SIZE), jnp.float32)
    return jnp.clip(values, -6.0, 6.0)


def draw_prefix_keys(key, part):
    return key_matrix(key).astype(jnp.bfloat16)


def draw_q_lat(key, part):
    drawn = jnp.clip(jax.random.normal(jax.random.fold_in(key, 7002), (TOKENS, H * DL), jnp.float32), -6.0, 6.0)
    return jnp.clip(drawn, -160.0, 160.0).astype(jnp.bfloat16)


def draw_comp_lengths(key, part):
    counts = CLEN // LBLK
    blocks = jax.random.randint(jax.random.fold_in(key, 7011), (COMPS,), 1, counts + 1)
    offset = jax.random.randint(jax.random.fold_in(key, 7012), (), 1, counts)
    other = (blocks[0] - 1 + offset) % counts + 1
    places = jnp.arange(COMPS, dtype=jnp.int32)
    blocks = jnp.where(places == 1, other, blocks)
    return (blocks * LBLK).astype(jnp.int32)


def steps_of(stream_key, dims, split, smallest, high):
    loudness = 1.0
    for position, shards_of in split:
        draws = jax.random.uniform(jax.random.fold_in(jax.random.fold_in(stream_key, 6), position), (shards_of,), jnp.float32, smallest / len(split), high / len(split))
        loudness = loudness * jnp.repeat(jnp.exp(draws), dims[position] // shards_of).reshape((-1,) + (1,) * (len(dims) - 1 - position))
    return loudness


def normal_values(stream_key, shape, deviation, limit, cuts=(), kind=jnp.bfloat16):
    level = steps_of(stream_key, shape, cuts, -0.22, 0.18) if cuts else 1.0
    result = jax.random.normal(stream_key, shape, jnp.float32) * deviation * level
    return jnp.minimum(jnp.maximum(result, -limit), limit).astype(kind)


def setup_inputs(seed: int = 0) -> dict:
    keys = jax.random.split(jax.random.key(seed), 7)
    return {
        "q_lat": draw_q_lat(jax.random.fold_in(keys[6], 71), 0),
        "q_rope": normal_values(keys[1], (TOKENS, H * DR), 1.0, 6.0, ((0, 32), (1, 8))),
        "grad_out": normal_values(keys[2], (TOKENS, H * DL), 1.0, 6.0, ((0, 32), (1, 8))),
        "prefix_keys": draw_prefix_keys(jax.random.fold_in(keys[6], 71), 0),
        "comp_lengths": draw_comp_lengths(jax.random.fold_in(keys[6], 71), 0),
        "prefix_len": jax.random.randint(keys[5], (1,), P_SIZE // 8 + 1, P_SIZE + 1).astype(jnp.int32),
    }


def reference(q_lat, q_rope, grad_out, prefix_keys, comp_lengths, prefix_len):
    scale = (DL + DR) ** -0.5
    tok_ids = jnp.arange(TOKENS, dtype=jnp.int32)
    length = comp_lengths[(tok_ids // CLEN).astype(jnp.int32)]
    valid = (tok_ids % CLEN) < length
    keep = jnp.arange(P_SIZE, dtype=jnp.int32) < prefix_len[0]
    key_lat = prefix_keys[:DL]
    key_rope = prefix_keys[DL:]
    upstream = jnp.where(valid[:, None], grad_out, jnp.zeros_like(grad_out))
    lat_heads = q_lat.reshape(TOKENS, H, DL).transpose(1, 0, 2)
    rope_heads = q_rope.reshape(TOKENS, H, DR).transpose(1, 0, 2)
    grad_heads = upstream.reshape(TOKENS, H, DL).transpose(1, 0, 2)
    contract_last = (((1,), (1,)), ((), ()))
    contract_first = (((0,), (0,)), ((), ()))

    def head_step(carry, inputs):
        query_lat, query_rope, upgrad = inputs
        scores = (jnp.dot(query_lat, key_lat, preferred_element_type=jnp.float32)
                  + jnp.dot(query_rope, key_rope, preferred_element_type=jnp.float32)) * scale
        scores = jnp.where(keep[None, :], scores, -jnp.inf)
        peak = jnp.max(scores, axis=1, keepdims=True)
        expo = jnp.exp(scores - peak)
        prob = expo / jnp.sum(expo, axis=1, keepdims=True)
        dprob = jnp.dot(upgrad, key_lat, preferred_element_type=jnp.float32)
        delta = jnp.sum(prob * dprob, axis=1, keepdims=True)
        dscore = prob * (dprob - delta)
        prob_b = prob.astype(jnp.bfloat16)
        dscore_b = dscore.astype(jnp.bfloat16)
        grad_lat = (scale * lax.dot_general(dscore_b, key_lat, contract_last, preferred_element_type=jnp.float32)).astype(jnp.bfloat16)
        grad_rope = (scale * lax.dot_general(dscore_b, key_rope, contract_last, preferred_element_type=jnp.float32)).astype(jnp.bfloat16)
        term_lat = (lax.dot_general(upgrad, prob_b, contract_first, preferred_element_type=jnp.float32)
                    + scale * lax.dot_general(query_lat, dscore_b, contract_first, preferred_element_type=jnp.float32))
        term_rope = scale * lax.dot_general(query_rope, dscore_b, contract_first, preferred_element_type=jnp.float32)
        carry = carry + jnp.concatenate([term_lat, term_rope], axis=0)
        return carry, (grad_lat, grad_rope)

    start = jnp.zeros((DL + DR, P_SIZE), jnp.float32)
    key_grads, outputs = lax.scan(head_step, start, (lat_heads, rope_heads, grad_heads))
    dq_lat = outputs[0].transpose(1, 0, 2).reshape(TOKENS, H * DL)
    dq_rope = outputs[1].transpose(1, 0, 2).reshape(TOKENS, H * DR)
    return (dq_lat, dq_rope, key_grads)
```

```python
import jax
import jax.numpy as jnp
from jax import lax
from jax.sharding import PartitionSpec as P

DL = 512
DR = 64
CLEN = 1024
AXES = ("dp", "seq", "head")
NX, NS, NH = 4, 8, 8
NZ = 8
NY = 4

neg_value = -1e30


def moved(dx=0, dy=0, dz=0, dc=0):
    pairs = []
    for x in range(NX):
        for s in range(NS):
            for h in range(NH):
                z = (h % 2) * 4 + s // 2
                tx, ty, tz, tc = (x + dx) % NX, (h // 2 + dy) % NY, (z + dz) % NZ, (s % 2) ^ dc
                src = (x * NS + s) * NH + h
                dst = (tx * NS + (tz % 4) * 2 + tc) * NH + ty * 2 + tz // 4
                pairs.append((src, dst))
    return pairs


def send(value, **shift):
    return lax.ppermute(value, AXES, moved(**shift))


def on_device(q_lat, q_rope, grad_out, prefix_keys, comp_lengths, prefix_len):
    tok_rows = q_lat.shape[0]
    heads_here = q_lat.shape[1] // DL
    rows = tok_rows * heads_here
    width = prefix_keys.shape[1]
    scale = (DL + DR) ** (-0.5)
    seq = lax.axis_index("seq")
    head = lax.axis_index("head")
    core = seq % 2
    zl = seq // 2
    y = head // 2
    zh = head % 2

    half = (DL + DR) // 2
    up_half = send(prefix_keys[:half], dz=2)
    down_half = send(prefix_keys[half:], dz=-2)
    from_below = send(prefix_keys, dz=1)
    from_above = send(prefix_keys, dz=-1)
    opposite = jnp.concatenate([up_half, down_half], axis=0)
    mine = jnp.concatenate([prefix_keys, from_above, from_below, opposite], axis=1)
    other = send(mine, dc=1)
    keys = jnp.concatenate([mine, other], axis=1)

    tok_ids = lax.axis_index(("dp", "seq")) * tok_rows + jnp.arange(tok_rows, dtype=jnp.int32)
    comp_ids = tok_ids // CLEN
    table = jnp.arange(comp_lengths.shape[0], dtype=jnp.int32)
    length = jnp.sum(
        jnp.where(comp_ids[:, None] == table[None, :], comp_lengths[None, :], 0), axis=1
    )
    valid = tok_ids % CLEN < length
    query_lat = q_lat.reshape(rows, DL)
    query_rope = q_rope.reshape(rows, DR)
    upstream = jnp.where(
        jnp.repeat(valid, heads_here)[:, None],
        grad_out.reshape(rows, DL),
        jnp.zeros((), jnp.bfloat16),
    )
    limit = prefix_len[0]

    shard_zl = jnp.array([0, 1, 3, 2], jnp.int32)
    shard_zl = (jnp.tile(shard_zl, 2) + zl) % 4
    shard_c = jnp.repeat(jnp.stack([core, 1 - core]), 4)
    base = (shard_zl * 2 + shard_c) * width
    cols = (base[:, None] + jnp.arange(width, dtype=jnp.int32)[None, :]).reshape(-1)
    keep = (cols < limit)[None, :]

    key_lat = keys[:DL]
    key_rope = keys[DL:]
    scores = (
        jnp.dot(query_lat, key_lat, preferred_element_type=jnp.float32)
        + jnp.dot(query_rope, key_rope, preferred_element_type=jnp.float32)
    ) * scale
    dprob = jnp.dot(upstream, key_lat, preferred_element_type=jnp.float32)
    masked = jnp.where(keep, scores, neg_value)
    peak = jnp.max(masked, axis=1)
    expo = jnp.where(keep, jnp.exp(masked - peak[:, None]), 0.0)
    total = jnp.sum(expo, axis=1)
    delta = jnp.sum(expo * dprob, axis=1) / total
    prob = expo / total[:, None]
    dscore_b = (prob * (dprob - delta[:, None])).astype(jnp.bfloat16)
    prob_b = prob.astype(jnp.bfloat16)

    first = (((0,), (0,)), ((), ()))
    last = (((1,), (1,)), ((), ()))
    term_lat = lax.dot_general(
        prob_b, upstream, first, preferred_element_type=jnp.float32
    ) + scale * lax.dot_general(dscore_b, query_lat, first, preferred_element_type=jnp.float32)
    term_rope = scale * lax.dot_general(
        dscore_b, query_rope, first, preferred_element_type=jnp.float32
    )
    update = jnp.concatenate([term_lat, term_rope], axis=1)
    n = 4 * width
    crossed = send(update[n:].astype(jnp.bfloat16), dc=1)
    chip = (update[:n] + crossed.astype(jnp.float32)).astype(jnp.bfloat16)
    q = width // 2
    opp = chip[3 * width :]
    low = send(opp[:q], dz=2)
    high = send(opp[q:], dz=-2)
    above = send(chip[width : 2 * width], dz=1)
    below = send(chip[2 * width : 3 * width], dz=-1)
    f32 = jnp.float32
    shard = (
        chip[:width].astype(f32)
        + above.astype(f32)
        + below.astype(f32)
        + jnp.concatenate([low, high], axis=0).astype(f32)
    ).astype(jnp.bfloat16)
    part = width // NY

    def slab(k):
        return lax.dynamic_slice_in_dim(shard, ((y + k) % NY) * part, part, 0)

    part_sum = slab(0).astype(f32)
    for k in (1, 3, 2):
        part_sum = part_sum + send(slab(k), dy=k).astype(f32)
    sub = part // 2
    to_send = lax.dynamic_slice_in_dim(part_sum, (1 - zh) * sub, sub, 0).astype(jnp.bfloat16)
    piece = lax.dynamic_slice_in_dim(part_sum, zh * sub, sub, 0) + send(to_send, dz=4).astype(f32)
    whole = piece
    for k in (1, 3, 2):
        whole = whole + send(piece, dx=k)
    d_keys = whole.T

    grad_lat = lax.dot_general(dscore_b, key_lat, last, preferred_element_type=jnp.float32)
    grad_rope = lax.dot_general(dscore_b, key_rope, last, preferred_element_type=jnp.float32)
    dq_lat = (scale * grad_lat).astype(jnp.bfloat16).reshape(tok_rows, heads_here * DL)
    dq_rope = (scale * grad_rope).astype(jnp.bfloat16).reshape(tok_rows, heads_here * DR)
    return (dq_lat, dq_rope, d_keys)


def solution(mesh):
    in_specs = (
        P(("dp", "seq"), "head"),
        P(("dp", "seq"), "head"),
        P(("dp", "seq"), "head"),
        P(None, "seq"),
        P(),
        P(),
    )
    out_specs = (P(("dp", "seq"), "head"), P(("dp", "seq"), "head"), P(None, ("seq", "head")))
    return jax.shard_map(
        on_device, mesh=mesh, in_specs=in_specs, out_specs=out_specs, check_vma=False
    )
```

```python
import functools
import math

import jax
import jax.numpy as jnp
from jax import lax
from jax.experimental import pallas as pl
from jax.experimental.pallas import tpu as pltpu
from jax.sharding import PartitionSpec as P

DL = 512
DR = 64
DK = DL + DR
CLEN = 1024
LBLK = 128
AXES = ("dp", "seq", "head")
NX, NS, NH = 4, 8, 8
NZ = 8
NY = 4
SCALE = DK ** (-0.5)
LOG2E = math.log2(math.e)
NEG = -1e30
STEPS = (0, 1, 3, 2)

f32 = jnp.float32
bf16 = jnp.bfloat16


def pairs_of(move):
    pairs = []
    for x in range(NX):
        for s in range(NS):
            for h in range(NH):
                z = (h % 2) * 4 + s // 2
                tx, ty, tz, tc = move(x, h // 2, z, s % 2)
                tz = tz % NZ
                src = (x * NS + s) * NH + h
                dst = ((tx % NX) * NS + (tz % 4) * 2 + tc) * NH + (ty % NY) * 2 + tz // 4
                pairs.append((src, dst))
    return pairs


def send(value, dx=0, dy=0, dz=0, dc=0):
    return lax.ppermute(
        value, AXES, pairs_of(lambda x, y, z, c: (x + dx, y + dy, z + dz, c ^ dc))
    )


def send_opposite(value):
    return lax.ppermute(
        value, AXES, pairs_of(lambda x, y, z, c: (x, y, z + 2 if z % 2 == 0 else z - 2, c))
    )


def chunk_bases(info, width):
    bases = []
    for flip in (0, 1):
        for step in STEPS:
            zl = (info[0] + step) % 4
            core = info[1] + flip * (1 - 2 * info[1])
            bases.append((zl * 2 + core) * width)
    return bases


def gradient_kernel(
    info, lens, q_ref, qr_ref, g_ref, k0, k1, k2, k3, k4, k5, k6, k7,
    own_ref, cross_ref, ds_ref,
    s_ref, d_ref, p_ref, gm_ref, qc_ref, gt_ref, qt_ref, m_ref, t_ref, w_ref,
):
    keys = (k0, k1, k2, k3, k4, k5, k6, k7)
    rows = q_ref.shape[0]
    heads = q_ref.shape[1] // DL
    width = k0.shape[1]
    limit = info[3]
    bases = chunk_bases(info, width)
    blocks = rows // LBLK

    for b in range(blocks):
        block = info[2] + b
        start = (block % (CLEN // LBLK)) * LBLK
        length = lens[block // (CLEN // LBLK)]
        row = lax.broadcasted_iota(jnp.int32, (LBLK, DL), 0) + start
        keep_row = row < length
        for h in range(heads):
            tile = g_ref[pl.ds(b * LBLK, LBLK), pl.ds(h * DL, DL)]
            gm_ref[pl.ds(h * rows + b * LBLK, LBLK), :] = jnp.where(
                keep_row, tile.astype(f32), 0.0
            ).astype(bf16)
    for h in range(heads):
        qc_ref[pl.ds(h * rows, rows), pl.ds(0, DL)] = q_ref[:, pl.ds(h * DL, DL)]
        qc_ref[pl.ds(h * rows, rows), pl.ds(DL, DR)] = qr_ref[:, h * DR : (h + 1) * DR]

    for h in range(heads):
        here = pl.ds(h * rows, rows)
        m_ref[...] = jnp.full(m_ref.shape, NEG, f32)
        for c in range(8):

            @pl.when(bases[c] < limit)
            def _(c=c, here=here):
                key = keys[c][...]
                s = jnp.dot(qc_ref[here, :], key, preferred_element_type=f32)
                col = lax.broadcasted_iota(jnp.int32, (1, width), 1) + bases[c]
                s = s * (SCALE * LOG2E) + jnp.where(col < limit, 0.0, NEG)
                s_ref[c] = s
                m_ref[...] = jnp.maximum(
                    m_ref[...], jnp.maximum(s[:, : width // 2], s[:, width // 2 :])
                )
                d_ref[c] = jnp.dot(gm_ref[here, :], key[:DL], preferred_element_type=f32)

        peak = jnp.max(m_ref[...], axis=1, keepdims=True)
        t_ref[...] = jnp.zeros(t_ref.shape, f32)
        w_ref[...] = jnp.zeros(w_ref.shape, f32)
        for c in range(8):

            @pl.when(bases[c] < limit)
            def _(c=c, peak=peak):
                e = jnp.exp2(s_ref[c] - peak)
                s_ref[c] = e
                ed = e * d_ref[c]
                t_ref[...] += e[:, : width // 2] + e[:, width // 2 :]
                w_ref[...] += ed[:, : width // 2] + ed[:, width // 2 :]

        total = jnp.sum(t_ref[...], axis=1, keepdims=True)
        delta = jnp.sum(w_ref[...], axis=1, keepdims=True) / total
        inv = 1.0 / total
        for c in range(8):

            @pl.when(bases[c] < limit)
            def _(c=c, here=here, inv=inv, delta=delta):
                p = s_ref[c] * inv
                p_ref[c, here, :] = p.astype(bf16)
                ds_ref[c, here, :] = (p * (d_ref[c] - delta)).astype(bf16)

    gt_ref[...] = gm_ref[...].T
    qt_ref[...] = qc_ref[...].T
    for c in (4, 5, 6, 7, 3, 1, 2, 0):
        out = own_ref.at[c] if c < 4 else cross_ref.at[c - 4]

        @pl.when(bases[c] < limit)
        def _(c=c, out=out):
            ds = ds_ref[c]
            low = jnp.dot(gt_ref[...], p_ref[c], preferred_element_type=f32)
            full = jnp.dot(qt_ref[...], ds, preferred_element_type=f32) * SCALE
            out[pl.ds(0, DL), :] = (low + full[:DL]).astype(out.dtype)
            out[pl.ds(DL, DR), :] = full[DL:].astype(out.dtype)

        @pl.when(bases[c] >= limit)
        def _(out=out):
            out[...] = jnp.zeros(out.shape, out.dtype)


def query_kernel(info, ds_ref, k0, k1, k2, k3, k4, k5, k6, k7, lat_ref, rope_ref, acc_ref):
    keys = (k0, k1, k2, k3, k4, k5, k6, k7)
    rows = lat_ref.shape[0]
    heads = lat_ref.shape[1] // DL
    width = k0.shape[1]
    bases = chunk_bases(info, width)
    acc_ref[...] = jnp.zeros(acc_ref.shape, f32)
    for c in range(8):

        @pl.when(bases[c] < info[3])
        def _(c=c):
            acc_ref[...] += lax.dot_general(
                ds_ref[c], keys[c][...], (((1,), (1,)), ((), ())), preferred_element_type=f32
            )

    ropes = []
    for h in range(heads):
        part = acc_ref[pl.ds(h * rows, rows), :] * SCALE
        lat_ref[:, pl.ds(h * DL, DL)] = part[:, :DL].astype(bf16)
        ropes.append(part[:, DL:])
    rope_ref[...] = jnp.concatenate(ropes, axis=1).astype(bf16)


def whole(n):
    return [pl.BlockSpec(memory_space=pltpu.VMEM)] * n


def on_device(q_lat, q_rope, grad_out, prefix_keys, comp_lengths, prefix_len):
    rows = q_lat.shape[0]
    heads = q_lat.shape[1] // DL
    width = prefix_keys.shape[1]
    seq = lax.axis_index("seq")
    head = lax.axis_index("head")
    y = head // 2
    zh = head % 2
    first_block = lax.axis_index(("dp", "seq")) * (rows // LBLK)
    info = jnp.stack([seq // 2, seq % 2, first_block, prefix_len[0]]).astype(jnp.int32)

    above = send(prefix_keys, dz=-1)
    below = send(prefix_keys, dz=1)
    opposite = send_opposite(prefix_keys)
    mine = (prefix_keys, above, below, opposite)
    keys = mine + tuple(send(k, dc=1) for k in mine)

    all_rows = rows * heads
    own, cross, ds = pl.pallas_call(
        gradient_kernel,
        out_shape=(
            jax.ShapeDtypeStruct((4, DK, width), f32),
            jax.ShapeDtypeStruct((4, DK, width), bf16),
            jax.ShapeDtypeStruct((8, all_rows, width), bf16),
        ),
        in_specs=[pl.BlockSpec(memory_space=pltpu.SMEM)] * 2 + whole(11),
        out_specs=tuple(whole(3)),
        scratch_shapes=[
            pltpu.VMEM((8, rows, width), f32),
            pltpu.VMEM((8, rows, width), f32),
            pltpu.VMEM((8, all_rows, width), bf16),
            pltpu.VMEM((all_rows, DL), bf16),
            pltpu.VMEM((all_rows, DK), bf16),
            pltpu.VMEM((DL, all_rows), bf16),
            pltpu.VMEM((DK, all_rows), bf16),
            pltpu.VMEM((rows, width // 2), f32),
            pltpu.VMEM((rows, width // 2), f32),
            pltpu.VMEM((rows, width // 2), f32),
        ],
        cost_estimate=pl.CostEstimate(
            flops=8 * all_rows * width * 2 * (DK + DL + DL + DK),
            transcendentals=8 * all_rows * width,
            bytes_accessed=12 << 20,
        ),
        name="prefix_gradient",
    )(info, comp_lengths, q_lat, q_rope, grad_out, *keys)

    crossed = send(cross, dc=1)
    chip = [own[c] + crossed[c].astype(f32) for c in range(4)]
    to_opposite = send_opposite(chip[3].astype(bf16))
    to_above = send(chip[1].astype(bf16), dz=1)
    to_below = send(chip[2].astype(bf16), dz=-1)

    lat, rope = pl.pallas_call(
        query_kernel,
        out_shape=(
            jax.ShapeDtypeStruct((rows, heads * DL), bf16),
            jax.ShapeDtypeStruct((rows, heads * DR), bf16),
        ),
        in_specs=[pl.BlockSpec(memory_space=pltpu.SMEM)] + whole(9),
        out_specs=tuple(whole(2)),
        scratch_shapes=[pltpu.VMEM((all_rows, DK), f32)],
        cost_estimate=pl.CostEstimate(
            flops=8 * all_rows * width * 2 * DK, transcendentals=0, bytes_accessed=7 << 20
        ),
        name="query_gradient",
    )(info, ds, *keys)

    shard = chip[0] + to_above.astype(f32) + to_below.astype(f32) + to_opposite.astype(f32)
    shard = shard.T.astype(bf16)
    part = width // NY

    def slab(k):
        return lax.dynamic_slice_in_dim(shard, ((y + k) % NY) * part, part, 0)

    part_sum = slab(0).astype(f32)
    for k in (1, 3, 2):
        part_sum = part_sum + send(slab(k), dy=k).astype(f32)
    sub = part // 2
    to_send = lax.dynamic_slice_in_dim(part_sum, (1 - zh) * sub, sub, 0).astype(bf16)
    piece = lax.dynamic_slice_in_dim(part_sum, zh * sub, sub, 0) + send(to_send, dz=4).astype(f32)
    summed = piece
    for k in (1, 3, 2):
        summed = summed + send(piece, dx=k)
    return (lat, rope, summed.T)


def solution(mesh):
    in_specs = (
        P(("dp", "seq"), "head"),
        P(("dp", "seq"), "head"),
        P(("dp", "seq"), "head"),
        P(None, "seq"),
        P(),
        P(),
    )
    out_specs = (P(("dp", "seq"), "head"), P(("dp", "seq"), "head"), P(None, ("seq", "head")))
    return jax.shard_map(
        on_device, mesh=mesh, in_specs=in_specs, out_specs=out_specs, check_vma=False
    )
```

```python
import functools
import math

import jax
import jax.numpy as jnp
from jax import lax
from jax.experimental import pallas as pl
from jax.experimental.pallas import tpu as pltpu
from jax.sharding import PartitionSpec as P

DL = 512
DR = 64
DK = DL + DR
CLEN = 1024
LBLK = 128
AXES = ("dp", "seq", "head")
NX, NS, NH = 4, 8, 8
NZ = 8
NY = 4
SCALE = DK ** (-0.5)
LOG2E = math.log2(math.e)
NEG = -1e30
STEPS = (0, 1, 3, 2)

f32 = jnp.float32
bf16 = jnp.bfloat16


def pairs_of(move):
    pairs = []
    for x in range(NX):
        for s in range(NS):
            for h in range(NH):
                z = (h % 2) * 4 + s // 2
                tx, ty, tz, tc = move(x, h // 2, z, s % 2)
                tz = tz % NZ
                src = (x * NS + s) * NH + h
                dst = ((tx % NX) * NS + (tz % 4) * 2 + tc) * NH + (ty % NY) * 2 + tz // 4
                pairs.append((src, dst))
    return pairs


def send(value, dx=0, dy=0, dz=0, dc=0):
    return lax.ppermute(
        value, AXES, pairs_of(lambda x, y, z, c: (x + dx, y + dy, z + dz, c ^ dc))
    )


def send_opposite(value):
    return lax.ppermute(
        value, AXES, pairs_of(lambda x, y, z, c: (x, y, z + 2 if z % 2 == 0 else z - 2, c))
    )


ZL, CORE, BLOCK, LIMIT, YPOS, ZHI = range(6)
SCOPED = 16 << 20


def base_of(info, c, width):
    zl = (info[ZL] + STEPS[c % 4]) % 4
    core = info[CORE] if c < 4 else 1 - info[CORE]
    return (zl * 2 + core) * width


def vmem_spec(n):
    return [pl.BlockSpec(memory_space=pltpu.VMEM)] * n


SMEM_SPEC = pl.BlockSpec(memory_space=pltpu.SMEM)


def local_call(kernel, outs, scalars, arrays, name, scratch=(), flops=0, nbytes=0):
    placed = [pltpu.with_memory_space_constraint(a, pltpu.VMEM) for a in arrays]
    return pl.pallas_call(
        kernel,
        out_shape=tuple(pltpu.VMEM(shape, dtype) for shape, dtype in outs),
        in_specs=[SMEM_SPEC] * len(scalars) + vmem_spec(len(placed)),
        out_specs=tuple(vmem_spec(len(outs))),
        scratch_shapes=list(scratch),
        compiler_params=pltpu.CompilerParams(vmem_limit_bytes=SCOPED),
        cost_estimate=pl.CostEstimate(flops=flops, transcendentals=0, bytes_accessed=nbytes),
        name=name,
    )(*scalars, *placed)


def prep_kernel(info, lens, q_ref, qr_ref, g_ref, qc_ref, gm_ref, gt_ref, qt_ref):
    rows = q_ref.shape[0]
    heads = q_ref.shape[1] // DL
    per_comp = CLEN // LBLK
    for b in range(rows // LBLK):
        block = info[BLOCK] + b
        length = lens[block // per_comp]
        row = lax.broadcasted_iota(jnp.int32, (LBLK, DL), 0) + (block % per_comp) * LBLK
        keep_row = row < length
        for h in range(heads):
            tile = g_ref[pl.ds(b * LBLK, LBLK), pl.ds(h * DL, DL)]
            gm_ref[pl.ds(h * rows + b * LBLK, LBLK), :] = jnp.where(
                keep_row, tile.astype(f32), 0.0
            ).astype(bf16)
    for h in range(heads):
        qc_ref[pl.ds(h * rows, rows), pl.ds(0, DL)] = q_ref[:, pl.ds(h * DL, DL)]
        qc_ref[pl.ds(h * rows, rows), pl.ds(DL, DR)] = qr_ref[:, h * DR : (h + 1) * DR]
    gt_ref[...] = gm_ref[...].T
    qt_ref[...] = qc_ref[...].T


def score_chunk(info, c, key_ref, qc_ref, gm_ref, s_ref, d_ref, m_ref):
    width = key_ref.shape[1]
    base = base_of(info, c, width)

    @pl.when(base < info[LIMIT])
    def _():
        key = key_ref[...]
        s = jnp.dot(qc_ref[...], key, preferred_element_type=f32)
        col = lax.broadcasted_iota(jnp.int32, (1, width), 1) + base
        s = s * (SCALE * LOG2E) + jnp.where(col < info[LIMIT], 0.0, NEG)
        s_ref[...] = s
        m_ref[...] = jnp.maximum(
            m_ref[...], jnp.maximum(s[:, : width // 2], s[:, width // 2 :])
        )
        d_ref[...] = jnp.dot(gm_ref[...], key[:DL], preferred_element_type=f32)


def scores_kernel(chunks, info, *refs):
    n = len(chunks)
    keys, (qc_ref, gm_ref) = refs[:n], refs[n : n + 2]
    s_refs, d_refs, m_ref = refs[n + 2 : 2 * n + 2], refs[2 * n + 2 : 3 * n + 2], refs[3 * n + 2]
    m_ref[...] = jnp.full(m_ref.shape, NEG, f32)
    for i, c in enumerate(chunks):
        score_chunk(info, c, keys[i], qc_ref, gm_ref, s_refs[i], d_refs[i], m_ref)


def stats_kernel(early, late, info, *refs):
    ne, nl = len(early), len(late)
    refs = list(refs)

    def take(n):
        out, refs[:] = refs[:n], refs[n:]
        return out

    keys = take(nl)
    (qc_ref, gm_ref) = take(2)
    s_early, d_early = take(ne), take(ne)
    (m_early,) = take(1)
    s_late, d_late = take(nl), take(nl)
    norm_ref, delta_ref = take(2)
    m_ref, t_ref, w_ref = take(3)
    width = keys[0].shape[1]
    m_ref[...] = m_early[...]
    for i, c in enumerate(late):
        score_chunk(info, c, keys[i], qc_ref, gm_ref, s_late[i], d_late[i], m_ref)
    peak = jnp.max(m_ref[...], axis=1, keepdims=True)
    m_ref[...] = jnp.broadcast_to(peak, m_ref.shape)
    t_ref[...] = jnp.zeros(t_ref.shape, f32)
    w_ref[...] = jnp.zeros(w_ref.shape, f32)
    for c, s_ref, d_ref in zip(
        early + late, s_early + s_late, d_early + d_late, strict=True
    ):

        @pl.when(base_of(info, c, width) < info[LIMIT])
        def _(s_ref=s_ref, d_ref=d_ref):
            half = width // 2
            peaks = m_ref[...]
            lo = jnp.exp2(s_ref[:, :half] - peaks)
            hi = jnp.exp2(s_ref[:, half:] - peaks)
            t_ref[...] += lo + hi
            w_ref[...] += lo * d_ref[:, :half] + hi * d_ref[:, half:]

    total = jnp.sum(t_ref[...], axis=1, keepdims=True)
    weighted = jnp.sum(w_ref[...], axis=1, keepdims=True)
    norm_ref[...] = jnp.broadcast_to(peak + jnp.log2(total), norm_ref.shape)
    delta_ref[...] = jnp.broadcast_to(weighted / total, delta_ref.shape)


def keys_kernel(chunks, info, *refs):
    n = len(chunks)
    s_refs, d_refs = refs[:n], refs[n : 2 * n]
    norm_ref, delta_ref, gt_ref, qt_ref = refs[2 * n : 2 * n + 4]
    outs, ds_refs = refs[2 * n + 4 : 3 * n + 4], refs[3 * n + 4 : 4 * n + 4]
    width = s_refs[0].shape[1]
    half = width // 2
    for i, c in enumerate(chunks):
        out = outs[i]
        base = base_of(info, c, width)

        @pl.when(base < info[LIMIT])
        def _(i=i, out=out):
            norm, delta = norm_ref[...], delta_ref[...]
            p, ds = [], []
            for k in range(2):
                at = pl.ds(k * half, half)
                prob = jnp.exp2(s_refs[i][:, at] - norm)
                p.append(prob.astype(bf16))
                ds.append((prob * (d_refs[i][:, at] - delta)).astype(bf16))
            p = jnp.concatenate(p, axis=1)
            ds = jnp.concatenate(ds, axis=1)
            ds_refs[i][...] = ds
            low = jnp.dot(gt_ref[...], p, preferred_element_type=f32)
            full = jnp.dot(qt_ref[...], ds, preferred_element_type=f32) * SCALE
            out[pl.ds(0, DL), :] = (low + full[:DL]).astype(out.dtype)
            out[pl.ds(DL, DR), :] = full[DL:].astype(out.dtype)

        @pl.when(base >= info[LIMIT])
        def _(out=out):
            out[...] = jnp.zeros(out.shape, out.dtype)


def query_kernel(chunks, info, *refs):
    n = len(chunks)
    ds_refs, keys = refs[:n], refs[n : 2 * n]
    lat_ref, rope_ref, acc_ref = refs[2 * n :]
    rows = lat_ref.shape[0]
    heads = lat_ref.shape[1] // DL
    width = keys[0].shape[1]
    acc_ref[...] = jnp.zeros(acc_ref.shape, f32)
    for i, c in enumerate(chunks):

        @pl.when(base_of(info, c, width) < info[LIMIT])
        def _(i=i):
            acc_ref[...] += lax.dot_general(
                ds_refs[i][...],
                keys[i][...],
                (((1,), (1,)), ((), ())),
                preferred_element_type=f32,
            )

    ropes = []
    for h in range(heads):
        part = acc_ref[pl.ds(h * rows, rows), :] * SCALE
        lat_ref[:, pl.ds(h * DL, DL)] = part[:, :DL].astype(bf16)
        ropes.append(part[:, DL:])
    rope_ref[...] = jnp.concatenate(ropes, axis=1).astype(bf16)


def chip_kernel(*refs):
    n = len(refs) // 3
    for own, crossed, out in zip(refs[:n], refs[n : 2 * n], refs[2 * n :], strict=True):
        out[...] = (own[...] + crossed[...].astype(f32)).astype(out.dtype)


def shard_kernel(info, own, crossed, r1, r2, r3, after, *refs):
    outs, turned = refs[:NY], refs[NY]
    total = own[...] + crossed[...].astype(f32)
    total = total + r1[...].astype(f32) + r2[...].astype(f32) + r3[...].astype(f32)
    turned[...] = total.T
    part = outs[0].shape[0]
    for k in range(NY):
        at = pl.multiple_of(((info[YPOS] + k) % NY) * part, part)
        outs[k][...] = turned[pl.ds(at, part), :].astype(outs[k].dtype)


def slab_kernel(info, kept, r1, r2, r3, keep_ref, send_ref, sum_ref):
    sum_ref[...] = (
        kept[...] + r1[...].astype(f32) + r2[...].astype(f32) + r3[...].astype(f32)
    )
    sub = keep_ref.shape[0]
    zh = info[ZHI]
    keep_ref[...] = sum_ref[pl.ds(pl.multiple_of(zh * sub, sub), sub), :]
    send_ref[...] = sum_ref[pl.ds(pl.multiple_of((1 - zh) * sub, sub), sub), :].astype(bf16)


def on_device(q_lat, q_rope, grad_out, prefix_keys, comp_lengths, prefix_len):
    rows = q_lat.shape[0]
    heads = q_lat.shape[1] // DL
    width = prefix_keys.shape[1]
    all_rows = rows * heads
    seq = lax.axis_index("seq")
    head = lax.axis_index("head")
    first_block = lax.axis_index(("dp", "seq")) * (rows // LBLK)
    info = jnp.stack(
        [seq // 2, seq % 2, first_block, prefix_len[0], head // 2, head % 2]
    ).astype(jnp.int32)

    partner = send(prefix_keys, dc=1)
    above = send(prefix_keys, dz=-1)
    below = send(prefix_keys, dz=1)
    opposite = send_opposite(prefix_keys)
    key = {0: prefix_keys, 1: above, 2: below, 3: opposite, 4: partner}
    for c in (1, 2, 3):
        key[c + 4] = send(key[c], dc=1)

    square = (all_rows, width)
    lanes = (all_rows, width // 2)
    chunk_flops = all_rows * width * 2 * DL
    qc, gm, gt, qt = local_call(
        prep_kernel,
        [
            ((all_rows, DK), bf16),
            ((all_rows, DL), bf16),
            ((DL, all_rows), bf16),
            ((DK, all_rows), bf16),
        ],
        (info, comp_lengths),
        (q_lat, q_rope, grad_out),
        "prep",
        flops=chunk_flops,
        nbytes=6 << 20,
    )
    early, late = [0, 4], [1, 5, 2, 6, 3, 7]
    ne, nl = len(early), len(late)
    *sd, peak = local_call(
        functools.partial(scores_kernel, early),
        [(square, f32)] * (2 * ne) + [(lanes, f32)],
        (info,),
        [key[c] for c in early] + [qc, gm],
        "scores",
        flops=2 * ne * chunk_flops,
        nbytes=6 << 20,
    )
    s = dict(zip(early, sd[:ne], strict=True))
    d = dict(zip(early, sd[ne:], strict=True))
    *sd, norm, delta = local_call(
        functools.partial(stats_kernel, early, late),
        [(square, f32)] * (2 * nl) + [(lanes, f32)] * 2,
        (info,),
        [key[c] for c in late]
        + [qc, gm]
        + [s[c] for c in early]
        + [d[c] for c in early]
        + [peak],
        "stats",
        scratch=[pltpu.VMEM(lanes, f32)] * 3,
        flops=2 * nl * chunk_flops,
        nbytes=12 << 20,
    )
    s.update(zip(late, sd[:nl], strict=True))
    d.update(zip(late, sd[nl:], strict=True))

    grads, ds = {}, {}
    for chunks, dtype, name in (((7, 5, 6, 4), bf16, "cross"), ((3, 1, 2, 0), f32, "own")):
        res = local_call(
            functools.partial(keys_kernel, chunks),
            [((DK, width), dtype)] * 4 + [(square, bf16)] * 4,
            (info,),
            [s[c] for c in chunks] + [d[c] for c in chunks] + [norm, delta, gt, qt],
            name,
            flops=2 * 4 * chunk_flops,
            nbytes=8 << 20,
        )
        grads.update(zip(chunks, res[:4], strict=True))
        ds.update(zip(chunks, res[4:], strict=True))

    crossed = {c: send(grads[c + 4], dc=1) for c in (3, 1, 2, 0)}
    chip = dict(
        zip(
            (3, 1, 2),
            local_call(
                chip_kernel,
                [((DK, width), bf16)] * 3,
                (),
                [grads[c] for c in (3, 1, 2)] + [crossed[c] for c in (3, 1, 2)],
                "chip",
                flops=chunk_flops // 8,
                nbytes=4 << 20,
            ),
            strict=True,
        )
    )
    arrived = (send_opposite(chip[3]), send(chip[1], dz=1), send(chip[2], dz=-1))

    order = tuple(range(8))
    lat, rope = pl.pallas_call(
        functools.partial(query_kernel, order),
        out_shape=(
            jax.ShapeDtypeStruct((rows, heads * DL), bf16),
            jax.ShapeDtypeStruct((rows, heads * DR), bf16),
        ),
        in_specs=[SMEM_SPEC] + vmem_spec(16),
        out_specs=tuple(vmem_spec(2)),
        scratch_shapes=[pltpu.VMEM((all_rows, DK), f32)],
        cost_estimate=pl.CostEstimate(
            flops=8 * chunk_flops, transcendentals=0, bytes_accessed=7 << 20
        ),
        compiler_params=pltpu.CompilerParams(vmem_limit_bytes=SCOPED),
        name="query",
    )(
        info,
        *[
            pltpu.with_memory_space_constraint(a, pltpu.VMEM)
            for a in [ds[c] for c in order] + [key[c] for c in order]
        ],
    )

    part = width // NY
    slabs = pl.pallas_call(
        shard_kernel,
        out_shape=(pltpu.VMEM((part, DK), f32),)
        + tuple(pltpu.VMEM((part, DK), bf16) for _ in range(NY - 1)),
        in_specs=[SMEM_SPEC] + vmem_spec(5) + [pl.BlockSpec(memory_space=pl.ANY)],
        out_specs=tuple(vmem_spec(NY)),
        scratch_shapes=[pltpu.VMEM((width, DK), f32)],
        compiler_params=pltpu.CompilerParams(vmem_limit_bytes=SCOPED),
        name="shard",
    )(
        info,
        *[
            pltpu.with_memory_space_constraint(a, pltpu.VMEM)
            for a in (grads[0], crossed[0], *arrived)
        ],
        rope,
    )
    sub = part // 2
    keep, give = local_call(
        slab_kernel,
        [((sub, DK), f32), ((sub, DK), bf16)],
        (info,),
        [slabs[0]] + [send(slabs[k], dy=k) for k in (1, 3, 2)],
        "slab",
        scratch=[pltpu.VMEM((part, DK), f32)],
    )
    piece = keep + send(give, dz=4).astype(f32)
    summed = piece
    for k in (1, 3, 2):
        summed = summed + send(piece, dx=k)
    return (lat, rope, summed.T)


def solution(mesh):
    in_specs = (
        P(("dp", "seq"), "head"),
        P(("dp", "seq"), "head"),
        P(("dp", "seq"), "head"),
        P(None, "seq"),
        P(),
        P(),
    )
    out_specs = (P(("dp", "seq"), "head"), P(("dp", "seq"), "head"), P(None, ("seq", "head")))
    return jax.shard_map(
        on_device, mesh=mesh, in_specs=in_specs, out_specs=out_specs, check_vma=False
    )
```
